32 devices in a mesh: ctx: 16 (over z, y, x), tp: 2 (over core).
Axes of the slice: x: 2, y: 2, z: 4, core: 2. Of those that a mesh axis runs over, the one named last changes fastest.
Arguments:
- hidden_states: bfloat16 [4096, 8192], P('ctx', 'tp'), may hold values from -6 to 6
- queries: bfloat16 [4096, 4096], P('ctx', 'tp')
- key_matrix: bfloat16 [8192, 1024], P('tp'), may hold values from -0.0625 to 0.0625
- value_matrix: bfloat16 [8192, 1024], P('tp'), may hold values from -0.0625 to 0.0625
- stretch_table: int32 [32], replicated, may hold values from 0 to 31, as said below
Outputs:
- attended: bfloat16 [4096, 4096], P('ctx', 'tp')
The draws below stay inside these ranges and needn't reach their ends.
Inputs may be any that keep to these rules, and one draw needn't show every extreme that they name: `stretch_table`: a permutation of 0 to 31 in which entries 2 i and 2 i + 1 are two stretches c and 31 - c.
All inputs are finite; a program needn't handle non-finite values.
Results may differ from the reference program's by a relative error of at most 0.007.
The reference program's roundings to bfloat16 on the way count: a program that leaves them out, or rounds other values in their place, can miss the bound.
Values may be sent and summed in bfloat16 or wider, within the bound.
A program may use at most 256 MiB of HBM per device.

```python
import jax
import jax.numpy as jnp
from jax import lax

MODEL_WIDTH = 8192
QUERY_HEADS = 32
KEY_VALUE_HEADS = 8
HEAD_SIZE = 128
STRETCH = 128
STRETCHES = 32
SEQUENCE_TOKENS = 4096


def draw_queries(key, part):
    value_rows = jax.random.normal(jax.random.fold_in(key, 11), (SEQUENCE_TOKENS, QUERY_HEADS * HEAD_SIZE), jnp.float32)
    value_rows = jnp.clip(value_rows, -6.0, 6.0)
    return value_rows.astype(jnp.bfloat16)


def draw_stretch_table(key, part):
    half = STRETCHES // 2
    order = jax.random.permutation(jax.random.fold_in(key, 21), half).astype(jnp.int32)
    flips = jax.random.randint(jax.random.fold_in(key, 22), (half,), 0, 2).astype(jnp.int32)
    first = jnp.where(flips == 1, STRETCHES - 1 - order, order)
    second = STRETCHES - 1 - first
    return jnp.stack([first, second], axis=1).reshape(STRETCHES).astype(jnp.int32)


def steps_of(own_key, extent, shards, low, top_value):
    gain = 1.0
    for axis_at, parts in shards:
        draws = jax.random.uniform(jax.random.fold_in(jax.random.fold_in(own_key, 6), axis_at), (parts,), jnp.float32, low / len(shards), top_value / len(shards))
        gain = gain * jnp.repeat(jnp.exp(draws), extent[axis_at] // parts).reshape((-1,) + (1,) * (len(extent) - 1 - axis_at))
    return gain


def centred(stream_key, extent, spread, reach, split=(), kind=jnp.bfloat16):
    entries = spread * jax.random.normal(stream_key, extent, jnp.float32)
    if split:
        entries = entries * steps_of(stream_key, extent, split, -0.22, 0.18)
    return jnp.clip(entries, -reach, reach).astype(kind)


def setup_inputs(seed: int = 0) -> dict:
    splits = jax.random.split(jax.random.key(seed), 6)
    return {
        "hidden_states": centred(splits[0], (SEQUENCE_TOKENS, MODEL_WIDTH), 1.0, 6.0, ((0, 16), (1, 2))),
        "queries": draw_queries(jax.random.fold_in(splits[5], 71), 0),
        "key_matrix": centred(splits[2], (MODEL_WIDTH, KEY_VALUE_HEADS * HEAD_SIZE), MODEL_WIDTH ** -0.5, 0.0625, ((0, 2),)),
        "value_matrix": centred(splits[3], (MODEL_WIDTH, KEY_VALUE_HEADS * HEAD_SIZE), MODEL_WIDTH ** -0.5, 0.0625, ((0, 2),)),
        "stretch_table": draw_stretch_table(jax.random.fold_in(splits[5], 71), 0),
    }


def reference(hidden_states, queries, key_matrix, value_matrix, stretch_table):
    key_rows = jnp.dot(hidden_states, key_matrix, preferred_element_type=jnp.float32).astype(jnp.bfloat16)
    value_rows = jnp.dot(hidden_states, value_matrix, preferred_element_type=jnp.float32).astype(jnp.bfloat16)
    offsets = jnp.arange(SEQUENCE_TOKENS, dtype=jnp.int32)
    position = (jnp.repeat(stretch_table.astype(jnp.int32), STRETCH) * STRETCH + offsets % STRETCH).astype(jnp.int32)
    key_tiles = key_rows.astype(jnp.float32).reshape(SEQUENCE_TOKENS, KEY_VALUE_HEADS, HEAD_SIZE)
    value_tiles = value_rows.astype(jnp.float32).reshape(SEQUENCE_TOKENS, KEY_VALUE_HEADS, HEAD_SIZE)
    group_ratio = QUERY_HEADS // KEY_VALUE_HEADS
    rows_per_block = 128 if SEQUENCE_TOKENS % 128 == 0 else SEQUENCE_TOKENS
    query_block_list = queries.reshape(SEQUENCE_TOKENS // rows_per_block, rows_per_block, KEY_VALUE_HEADS, group_ratio, HEAD_SIZE)
    query_places = position.reshape(SEQUENCE_TOKENS // rows_per_block, rows_per_block)
    scale = 1.0 / (HEAD_SIZE ** 0.5)

    def one_block(items):
        query_block, places = items
        score = jnp.einsum('tgrd,ngd->grtn', query_block.astype(jnp.float32), key_tiles) * scale
        visible = position[None, :] <= places[:, None]
        masked = jnp.where(visible, score, jnp.float32(-1e30))
        highest = jnp.max(masked, axis=-1, keepdims=True)
        weight = jnp.where(visible, jnp.exp(masked - highest), jnp.float32(0.0))
        total = jnp.sum(weight, axis=-1)
        rounded = lax.optimization_barrier(weight.astype(jnp.bfloat16)).astype(jnp.float32)
        output = jnp.einsum('grtn,ngd->grtd', rounded, value_tiles) / total[..., None]
        return output.transpose(2, 0, 1, 3).reshape(rows_per_block, QUERY_HEADS * HEAD_SIZE).astype(jnp.bfloat16)

    outputs = lax.map(one_block, (query_block_list, query_places))
    return outputs.reshape(SEQUENCE_TOKENS, QUERY_HEADS * HEAD_SIZE)
```

```python
import functools

import jax
import jax.numpy as jnp
from jax import lax
from jax.experimental import pallas as pl
from jax.experimental.pallas import tpu as pltpu
from jax.sharding import PartitionSpec as P

KEY_VALUE_HEADS = 8
HEAD_SIZE = 128
D = HEAD_SIZE
ROWS = 256
NEG = -1e30
LOG2E = 1.4426950408889634
MESH = pl.DeviceIdType.MESH


def kernel(
    G, R, B, S,
    table, hid_hbm, q_hbm, wk_hbm, wv_hbm, out_hbm,
    hid, w, part_send, part_recv, stage, kv, q_buf, qs, kcat, vcat, acc, mx, ls, o_send,
    hid_sem, w_sem, part_ssem, part_rsem, a2a_ssem, kv_sem, ring_ssem, q_ssem, q_rsem, q_lsem,
    o_ssem, o_rsem, o_lsem,
):
    me = lax.axis_index("ctx")
    tp = lax.axis_index("tp")
    zi = me // G
    ji = me % G
    other = 1 - tp
    up = (zi + 1) % B * G + ji
    down = (zi + B - 1) % B * G + ji
    half_ring = B // 2
    qw = R * D

    order = list(range(1, G)) + [0]

    def fetch(n, k, group):
        col = pl.multiple_of((group * G + (ji + k) % G) * D, D)
        a = pltpu.make_async_copy(wk_hbm.at[:, pl.ds(col, D)], w.at[n, :, pl.ds(0, D)], w_sem.at[n, 0])
        b = pltpu.make_async_copy(wv_hbm.at[:, pl.ds(col, D)], w.at[n, :, pl.ds(D, D)], w_sem.at[n, 1])
        return a, b

    hid_copy = pltpu.make_async_copy(hid_hbm, hid, hid_sem)
    hid_copy.start()
    fetches = []
    for i, k in enumerate(order):
        for which in range(2):
            pair = fetch(2 * i + which, k, other if which == 0 else tp)
            pair[0].start()
            pair[1].start()
            fetches.append(pair)

    barrier = pltpu.get_barrier_semaphore()
    for k in range(1, G):
        pl.semaphore_signal(barrier, inc=1, device_id=(zi * G + (ji + k) % G, tp), device_id_type=MESH)
    pl.semaphore_signal(barrier, inc=1, device_id=(me, other), device_id_type=MESH)
    pl.semaphore_signal(barrier, inc=1, device_id=(up, tp), device_id_type=MESH)
    pl.semaphore_signal(barrier, inc=1, device_id=(down, tp), device_id_type=MESH)
    pl.semaphore_wait(barrier, G + 2)

    def q_copy(k, h):
        p = (ji + k) % G
        return pltpu.make_async_remote_copy(
            src_ref=q_hbm.at[pl.ds(h * S, S), pl.ds(pl.multiple_of(p * qw, qw), qw)],
            dst_ref=q_buf.at[ji, h],
            send_sem=q_ssem.at[k, h],
            recv_sem=q_rsem.at[k, h],
            device_id=(zi * G + p, tp),
            device_id_type=MESH,
        )

    def q_own(h):
        return pltpu.make_async_copy(
            q_hbm.at[pl.ds(h * S, S), pl.ds(pl.multiple_of(ji * qw, qw), qw)], q_buf.at[ji, h], q_lsem.at[h]
        )

    for h in range(2):
        q_own(h).start()
    q_copy(1, 0).start()
    q_copy(G - 1, 0).start()

    def ring_copy(z, j, s, way):
        return pltpu.make_async_remote_copy(
            src_ref=kv.at[z, j],
            dst_ref=kv.at[z, j],
            send_sem=ring_ssem.at[way, s, j],
            recv_sem=kv_sem.at[z, j],
            device_id=(up if way == 0 else down, tp),
            device_id_type=MESH,
        )

    def ring_send(z, j, s, way):
        if s < half_ring - 1:
            ring_copy(z, j, s, way).start()
        else:
            @pl.when((j < G // 2) if way == 0 else (j >= G // 2))
            def _():
                ring_copy(z, j, s, way).start()

    def ring_done(z, j, s, way):
        if s < half_ring - 1:
            ring_copy(z, j, s, way).wait_send()
        else:
            @pl.when((j < G // 2) if way == 0 else (j >= G // 2))
            def _():
                ring_copy(z, j, s, way).wait_send()

    def wait_piece(z, j):
        ring_copy(z, j, 0, 0).wait_recv()

    def part_copy(i):
        return pltpu.make_async_remote_copy(
            src_ref=part_send.at[i],
            dst_ref=part_recv.at[i],
            send_sem=part_ssem.at[i],
            recv_sem=part_rsem.at[i],
            device_id=(me, other),
            device_id_type=MESH,
        )

    def a2a_copy(i, k):
        return pltpu.make_async_remote_copy(
            src_ref=stage.at[i],
            dst_ref=kv.at[zi, ji],
            send_sem=a2a_ssem.at[i],
            recv_sem=kv_sem.at[zi, ji],
            device_id=(zi * G + (ji + k) % G, tp),
            device_id_type=MESH,
        )

    hid_copy.wait()
    for i, k in enumerate(order):
        for n in (2 * i, 2 * i + 1):
            fetches[n][0].wait()
            fetches[n][1].wait()
            term = jnp.dot(hid[...], w[n], preferred_element_type=jnp.float32)
            if n % 2 == 0:
                part_send[i] = term
                part_copy(i).start()
            else:
                part_copy(i).wait_recv()
                both = (term + part_recv[i]).astype(jnp.bfloat16)
                for c in range(2):
                    for h in range(2):
                        block = both[h * S:(h + 1) * S, c * D:(c + 1) * D]
                        if k:
                            stage[i, c, h] = block
                        else:
                            kv[zi, ji, c, h] = block
        if k:
            a2a_copy(i, k).start()
        if i == len(order) - 2:
            for kk in range(1, G):
                for h in range(2):
                    if not (h == 0 and kk in (1, G - 1)):
                        q_copy(kk, h).start()
        if i:
            j = (ji + G - order[i - 1]) % G
            wait_piece(zi, j)
            for way in range(2):
                ring_send(zi, j, 0, way)
        if not k:
            for way in range(2):
                ring_send(zi, ji, 0, way)

    def flipped(z, j):
        return table[2 * (z * G + j)] > table[2 * (z * G + j) + 1]

    def ids(z, j):
        a = table[2 * (z * G + j)]
        b = table[2 * (z * G + j) + 1]
        return jnp.minimum(a, b), jnp.maximum(a, b)

    def sort_queries(j):
        flip = flipped(zi, j)
        first = q_buf[j, 0]
        second = q_buf[j, 1]
        low = jnp.where(flip, second, first)
        high = jnp.where(flip, first, second)
        for r in range(R):
            qs[j, 0, r * S:(r + 1) * S] = low[:, r * D:(r + 1) * D]
            qs[j, 1, r * S:(r + 1) * S] = high[:, r * D:(r + 1) * D]

    for h in range(2):
        q_own(h).wait()
    sort_queries(ji)

    rows_all = R * S
    rows_at = min(ROWS, rows_all)
    scale2 = LOG2E / D**0.5

    def gather_group(z):
        for j in range(G):
            flip = flipped(z, j)
            for c, cat in ((0, kcat), (1, vcat)):
                first = kv[z, j, c, 0]
                second = kv[z, j, c, 1]
                cat[0, j * S:(j + 1) * S] = jnp.where(flip, second, first)
                cat[1, j * S:(j + 1) * S] = jnp.where(flip, first, second)

    def unit(z, jq, h, at, first):
        rows = pl.ds(pl.multiple_of(at * rows_at, rows_at), rows_at)
        qx = qs[jq, h, rows]
        tq = ids(zi, jq)[h]
        row = lax.broadcasted_iota(jnp.int32, (rows_at, S), 0) % S
        col = lax.broadcasted_iota(jnp.int32, (rows_at, S), 1)
        diff = col - row
        pieces = []
        for side in range(h + 1):
            s = lax.dot_general(
                qx, kcat[side], (((1,), (1,)), ((), ())), preferred_element_type=jnp.float32
            )
            for j in range(G):
                block = s[:, j * S:(j + 1) * S]
                if side == h:
                    tk = ids(z, j)[side]
                    block = jnp.where(diff <= (tq - tk) * S, block, jnp.float32(NEG))
                pieces.append(block)
        top = pieces[0]
        for block in pieces[1:]:
            top = jnp.maximum(top, block)
        top = jnp.max(top, axis=1, keepdims=True)
        if first:
            new = jnp.broadcast_to(top, (rows_at, D))
        else:
            old = mx[jq, h, rows]
            new = jnp.maximum(old, top)
        shift = new * scale2
        weights = [jnp.exp2(block * scale2 - shift) for block in pieces]
        total = weights[0]
        for weight in weights[1:]:
            total = total + weight
        value = None
        for side in range(h + 1):
            weight = jnp.concatenate(
                [x.astype(jnp.bfloat16) for x in weights[side * G:(side + 1) * G]], axis=1
            )
            term = jnp.dot(weight, vcat[side], preferred_element_type=jnp.float32)
            value = term if value is None else value + term
        if first:
            acc[jq, h, rows] = value
            ls[jq, h, rows] = total
        else:
            factor = jnp.exp2(old * scale2 - shift)
            acc[jq, h, rows] = acc[jq, h, rows] * factor + value
            ls[jq, h, rows] = ls[jq, h, rows] * factor + total
        mx[jq, h, rows] = new

    def visit_one(z, jq, first):
        def step(at, _):
            for h in range(2):
                unit(z, jq, h, at, first)
            return 0

        lax.fori_loop(0, rows_all // rows_at, step, 0)

    for h in range(2):
        pass
    gather_group(zi)
    visit_one(zi, ji, True)
    for k in range(1, G):
        for h in range(2):
            q_copy(k, h).wait_recv()
        sort_queries((ji + G - k) % G)

    def visit(z, first):
        def step(k, _):
            visit_one(z, (ji + k) % G, first)
            return 0

        lax.fori_loop(1 if first else 0, G, step, 0)

    visit(zi, True)

    for s in range(1, half_ring):
        below = (zi + B - s) % B
        above = (zi + s) % B
        if s < half_ring - 1:
            for j in range(G):
                wait_piece(below, j)
                ring_send(below, j, s, 0)
                wait_piece(above, j)
                ring_send(above, j, s, 1)
        else:
            for j in range(G // 2):
                wait_piece(below, j)
                ring_copy(below, j, s, 0).start()
                wait_piece(above, j + G // 2)
                ring_copy(above, j + G // 2, s, 1).start()
            for j in range(G // 2):
                wait_piece(below, j + G // 2)
        gather_group(below)
        visit(below, False)
        if s == half_ring - 1:
            for j in range(G // 2):
                wait_piece(above, j)
        gather_group(above)
        visit(above, False)

    def o_copy(k):
        p = (ji + k) % G
        return pltpu.make_async_remote_copy(
            src_ref=o_send.at[k],
            dst_ref=out_hbm.at[:, pl.ds(pl.multiple_of(ji * qw, qw), qw)],
            send_sem=o_ssem.at[k],
            recv_sem=o_rsem.at[k],
            device_id=(zi * G + p, tp),
            device_id_type=MESH,
        )

    last = (zi + half_ring) % B
    for j in range(G):
        wait_piece(last, j)
    gather_group(last)

    def finish(k):
        jq = (ji + k) % G
        visit_one(last, jq, False)
        flip = flipped(zi, jq)
        for r in range(R):
            rows = slice(r * S, (r + 1) * S)
            ends = [
                (acc[jq, h, rows] / jnp.sum(ls[jq, h, rows], axis=1, keepdims=True)).astype(jnp.bfloat16)
                for h in range(2)
            ]
            o_send[k, 0:S, r * D:(r + 1) * D] = jnp.where(flip, ends[1], ends[0])
            o_send[k, S:2 * S, r * D:(r + 1) * D] = jnp.where(flip, ends[0], ends[1])

    def finish_step(k, _):
        finish(k)
        o_copy(k).start()
        return 0

    lax.fori_loop(1, G, finish_step, 0)
    finish(0)
    mine = pltpu.make_async_copy(
        o_send.at[0], out_hbm.at[:, pl.ds(pl.multiple_of(ji * qw, qw), qw)], o_lsem
    )
    mine.start()

    for i, k in enumerate(order):
        part_copy(i).wait_send()
        if k:
            a2a_copy(i, k).wait_send()
            for h in range(2):
                q_copy(k, h).wait_send()
    for s in range(half_ring):
        for j in range(G):
            jj = (ji + j) % G
            ring_done((zi + B - s) % B, jj, s, 0)
            ring_done((zi + s) % B, jj, s, 1)
    for k in range(1, G):
        o_copy(k).wait_send()
        o_copy(k).wait_recv()
    mine.wait()


def body(hidden_states, queries, key_matrix, value_matrix, stretch_table):
    tokens, width = hidden_states.shape
    G = KEY_VALUE_HEADS // lax.axis_size("tp")
    ctx = lax.axis_size("ctx")
    B = ctx // G
    S = tokens // 2
    R = queries.shape[1] // (G * D)
    any_ = pl.BlockSpec(memory_space=pl.ANY)
    bf, f32 = jnp.bfloat16, jnp.float32
    dma = pltpu.SemaphoreType.DMA
    return pl.pallas_call(
        functools.partial(kernel, G, R, B, S),
        out_shape=jax.ShapeDtypeStruct(queries.shape, bf),
        in_specs=[pl.BlockSpec(memory_space=pltpu.SMEM)] + [any_] * 4,
        out_specs=any_,
        scratch_shapes=[
            pltpu.VMEM((tokens, width), bf),
            pltpu.VMEM((2 * G, width, 2 * D), bf),
            pltpu.VMEM((G, tokens, 2 * D), f32),
            pltpu.VMEM((G, tokens, 2 * D), f32),
            pltpu.VMEM((G, 2, 2, S, D), bf),
            pltpu.VMEM((B, G, 2, 2, S, D), bf),
            pltpu.VMEM((G, 2, S, R * D), bf),
            pltpu.VMEM((G, 2, R * S, D), bf),
            pltpu.VMEM((2, G * S, D), bf),
            pltpu.VMEM((2, G * S, D), bf),
            pltpu.VMEM((G, 2, R * S, D), f32),
            pltpu.VMEM((G, 2, R * S, D), f32),
            pltpu.VMEM((G, 2, R * S, D), f32),
            pltpu.VMEM((G, tokens, R * D), bf),
            dma,
            dma((2 * G, 2)),
            dma((G,)),
            dma((G,)),
            dma((G,)),
            dma((B, G)),
            dma((2, B // 2, G)),
            dma((G, 2)),
            dma((G, 2)),
            dma((2,)),
            dma((G,)),
            dma((G,)),
            dma,
        ],
        compiler_params=pltpu.CompilerParams(
            collective_id=0, has_side_effects=True, vmem_limit_bytes=60 * 1024 * 1024
        ),
        name="fused",
    )(stretch_table, hidden_states, queries, key_matrix, value_matrix)


def solution(mesh):
    in_specs = (P("ctx", "tp"), P("ctx", "tp"), P("tp", None), P("tp", None), P())
    out_specs = P("ctx", "tp")
    return jax.shard_map(body, mesh=mesh, in_specs=in_specs, out_specs=out_specs, check_vma=False)
```

```python
import functools

import jax
import jax.numpy as jnp
from jax import lax
from jax.experimental import pallas as pl
from jax.experimental.pallas import tpu as pltpu
from jax.sharding import PartitionSpec as P

KEY_VALUE_HEADS = 8
HEAD_SIZE = 128
D = HEAD_SIZE
ROWS = 256
NEG = -1e30
LOG2E = 1.4426950408889634
MESH = pl.DeviceIdType.MESH


def kernel(
    G, R, B, S,
    table, hid_hbm, q_hbm, wk_hbm, wv_hbm, out_hbm,
    hid, w, part_send, part_recv, stage, kv, q_buf, qs, kcat, vcat, acc, mx, ls, o_send,
    hid_sem, w_sem, part_ssem, part_rsem, a2a_ssem, kv_sem, ring_ssem, q_ssem, q_rsem, q_lsem,
    o_ssem, o_rsem, o_lsem,
):
    me = lax.axis_index("ctx")
    tp = lax.axis_index("tp")
    zi = me // G
    ji = me % G
    other = 1 - tp
    up = (zi + 1) % B * G + ji
    down = (zi + B - 1) % B * G + ji
    half_ring = B // 2

    def partner(k):
        return (ji + k % 2 * (1 - 2 * (ji % 2)) + k - k % 2) % G

    qw = R * D

    order = list(range(G - 1, -1, -1))

    def fetch(n, k, group):
        col = pl.multiple_of((group * G + partner(k)) * D, D)
        a = pltpu.make_async_copy(wk_hbm.at[:, pl.ds(col, D)], w.at[n, :, pl.ds(0, D)], w_sem.at[n, 0])
        b = pltpu.make_async_copy(wv_hbm.at[:, pl.ds(col, D)], w.at[n, :, pl.ds(D, D)], w_sem.at[n, 1])
        return a, b

    hid_copy = pltpu.make_async_copy(hid_hbm, hid, hid_sem)
    hid_copy.start()
    fetches = []
    for i, k in enumerate(order):
        for which in range(2):
            pair = fetch(2 * i + which, k, other if which == 0 else tp)
            pair[0].start()
            pair[1].start()
            fetches.append(pair)

    barrier = pltpu.get_barrier_semaphore()
    for k in range(1, G):
        pl.semaphore_signal(barrier, inc=1, device_id=(zi * G + partner(k), tp), device_id_type=MESH)
    pl.semaphore_signal(barrier, inc=1, device_id=(me, other), device_id_type=MESH)
    pl.semaphore_signal(barrier, inc=1, device_id=(up, tp), device_id_type=MESH)
    pl.semaphore_signal(barrier, inc=1, device_id=(down, tp), device_id_type=MESH)
    pl.semaphore_wait(barrier, G + 2)

    def q_copy(k, h):
        p = partner(k)
        return pltpu.make_async_remote_copy(
            src_ref=q_hbm.at[pl.ds(h * S, S), pl.ds(pl.multiple_of(p * qw, qw), qw)],
            dst_ref=q_buf.at[ji, h],
            send_sem=q_ssem.at[k, h],
            recv_sem=q_rsem.at[k, h],
            device_id=(zi * G + p, tp),
            device_id_type=MESH,
        )

    def q_own(h):
        return pltpu.make_async_copy(
            q_hbm.at[pl.ds(h * S, S), pl.ds(pl.multiple_of(ji * qw, qw), qw)], q_buf.at[ji, h], q_lsem.at[h]
        )

    for h in range(2):
        q_own(h).start()
    q_copy(1, 0).start()
    q_copy(2, 0).start()

    def ring_copy(z, j, s, way):
        return pltpu.make_async_remote_copy(
            src_ref=kv.at[z, j],
            dst_ref=kv.at[z, j],
            send_sem=ring_ssem.at[way, s, j],
            recv_sem=kv_sem.at[z, j],
            device_id=(up if way == 0 else down, tp),
            device_id_type=MESH,
        )

    def ring_send(z, j, s, way):
        if s < half_ring - 1:
            ring_copy(z, j, s, way).start()
        else:
            @pl.when((j < G // 2) if way == 0 else (j >= G // 2))
            def _():
                ring_copy(z, j, s, way).start()

    def ring_done(z, j, s, way):
        if s < half_ring - 1:
            ring_copy(z, j, s, way).wait_send()
        else:
            @pl.when((j < G // 2) if way == 0 else (j >= G // 2))
            def _():
                ring_copy(z, j, s, way).wait_send()

    def wait_piece(z, j):
        ring_copy(z, j, 0, 0).wait_recv()

    def part_copy(i):
        return pltpu.make_async_remote_copy(
            src_ref=part_send.at[i],
            dst_ref=part_recv.at[i],
            send_sem=part_ssem.at[i],
            recv_sem=part_rsem.at[i],
            device_id=(me, other),
            device_id_type=MESH,
        )

    def a2a_copy(i, k):
        return pltpu.make_async_remote_copy(
            src_ref=stage.at[i],
            dst_ref=kv.at[zi, ji],
            send_sem=a2a_ssem.at[i],
            recv_sem=kv_sem.at[zi, ji],
            device_id=(zi * G + partner(k), tp),
            device_id_type=MESH,
        )

    hid_copy.wait()
    for i, k in enumerate(order):
        for n in (2 * i, 2 * i + 1):
            fetches[n][0].wait()
            fetches[n][1].wait()
            term = jnp.dot(hid[...], w[n], preferred_element_type=jnp.float32)
            if n % 2 == 0:
                part_send[i] = term
                part_copy(i).start()
            else:
                part_copy(i).wait_recv()
                both = (term + part_recv[i]).astype(jnp.bfloat16)
                for c in range(2):
                    for h in range(2):
                        block = both[h * S:(h + 1) * S, c * D:(c + 1) * D]
                        if k:
                            stage[i, c, h] = block
                        else:
                            kv[zi, ji, c, h] = block
        if k:
            a2a_copy(i, k).start()
        if i == len(order) - 2:
            for kk in range(1, G):
                for h in range(2):
                    if not (h == 0 and kk in (1, 2)):
                        q_copy(kk, h).start()
        if i:
            j = partner(order[i - 1])
            wait_piece(zi, j)
            for way in range(2):
                ring_send(zi, j, 0, way)
        if not k:
            for way in range(2):
                ring_send(zi, ji, 0, way)

    def flipped(z, j):
        return table[2 * (z * G + j)] > table[2 * (z * G + j) + 1]

    def ids(z, j):
        a = table[2 * (z * G + j)]
        b = table[2 * (z * G + j) + 1]
        return jnp.minimum(a, b), jnp.maximum(a, b)

    def sort_queries(j):
        flip = flipped(zi, j)
        first = q_buf[j, 0]
        second = q_buf[j, 1]
        low = jnp.where(flip, second, first)
        high = jnp.where(flip, first, second)
        for r in range(R):
            qs[j, 0, r * S:(r + 1) * S] = low[:, r * D:(r + 1) * D]
            qs[j, 1, r * S:(r + 1) * S] = high[:, r * D:(r + 1) * D]

    for h in range(2):
        q_own(h).wait()
    sort_queries(ji)

    rows_all = R * S
    rows_at = min(ROWS, rows_all)
    scale2 = LOG2E / D**0.5

    def gather_group(z):
        for j in range(G):
            flip = flipped(z, j)
            for c, cat in ((0, kcat), (1, vcat)):
                first = kv[z, j, c, 0]
                second = kv[z, j, c, 1]
                cat[0, j * S:(j + 1) * S] = jnp.where(flip, second, first)
                cat[1, j * S:(j + 1) * S] = jnp.where(flip, first, second)

    def unit(z, jq, h, at, first):
        rows = pl.ds(pl.multiple_of(at * rows_at, rows_at), rows_at)
        qx = qs[jq, h, rows]
        tq = ids(zi, jq)[h]
        row = lax.broadcasted_iota(jnp.int32, (rows_at, S), 0) % S
        col = lax.broadcasted_iota(jnp.int32, (rows_at, S), 1)
        diff = col - row
        pieces = []
        for side in range(h + 1):
            s = lax.dot_general(
                qx, kcat[side], (((1,), (1,)), ((), ())), preferred_element_type=jnp.float32
            )
            for j in range(G):
                block = s[:, j * S:(j + 1) * S]
                if side == h:
                    tk = ids(z, j)[side]
                    block = jnp.where(diff <= (tq - tk) * S, block, jnp.float32(NEG))
                pieces.append(block)
        top = pieces[0]
        for block in pieces[1:]:
            top = jnp.maximum(top, block)
        top = jnp.max(top, axis=1, keepdims=True)
        if first:
            new = jnp.broadcast_to(top, (rows_at, D))
        else:
            old = mx[jq, h, rows]
            new = jnp.maximum(old, top)
        shift = new * scale2
        weights = [jnp.exp2(block * scale2 - shift) for block in pieces]
        total = weights[0]
        for weight in weights[1:]:
            total = total + weight
        value = None
        for side in range(h + 1):
            weight = jnp.concatenate(
                [x.astype(jnp.bfloat16) for x in weights[side * G:(side + 1) * G]], axis=1
            )
            term = jnp.dot(weight, vcat[side], preferred_element_type=jnp.float32)
            value = term if value is None else value + term
        if first:
            acc[jq, h, rows] = value
            ls[jq, h, rows] = total
        else:
            factor = jnp.exp2(old * scale2 - shift)
            acc[jq, h, rows] = acc[jq, h, rows] * factor + value
            ls[jq, h, rows] = ls[jq, h, rows] * factor + total
        mx[jq, h, rows] = new

    def visit_one(z, jq, first):
        def step(at, _):
            for h in range(2):
                unit(z, jq, h, at, first)
            return 0

        lax.fori_loop(0, rows_all // rows_at, step, 0)

    for h in range(2):
        pass
    gather_group(zi)
    visit_one(zi, ji, True)
    for k in range(1, G):
        for h in range(2):
            q_copy(k, h).wait_recv()
        sort_queries(partner(k))

    def visit(z, first):
        def step(k, _):
            visit_one(z, partner(k), first)
            return 0

        lax.fori_loop(1 if first else 0, G, step, 0)

    visit(zi, True)

    for s in range(1, half_ring):
        below = (zi + B - s) % B
        above = (zi + s) % B
        if s < half_ring - 1:
            for j in range(G):
                wait_piece(below, j)
                ring_send(below, j, s, 0)
                wait_piece(above, j)
                ring_send(above, j, s, 1)
        else:
            for j in range(G // 2):
                wait_piece(below, j)
                ring_copy(below, j, s, 0).start()
                wait_piece(above, j + G // 2)
                ring_copy(above, j + G // 2, s, 1).start()
            for j in range(G // 2):
                wait_piece(below, j + G // 2)
        gather_group(below)
        visit(below, False)
        if s == half_ring - 1:
            for j in range(G // 2):
                wait_piece(above, j)
        gather_group(above)
        visit(above, False)

    def o_copy(k):
        p = partner(k)
        return pltpu.make_async_remote_copy(
            src_ref=o_send.at[k],
            dst_ref=out_hbm.at[:, pl.ds(pl.multiple_of(ji * qw, qw), qw)],
            send_sem=o_ssem.at[k],
            recv_sem=o_rsem.at[k],
            device_id=(zi * G + p, tp),
            device_id_type=MESH,
        )

    last = (zi + half_ring) % B
    for j in range(G):
        wait_piece(last, j)
    gather_group(last)

    def finish(k):
        jq = partner(k)
        visit_one(last, jq, False)
        flip = flipped(zi, jq)
        for r in range(R):
            rows = slice(r * S, (r + 1) * S)
            ends = [
                (acc[jq, h, rows] / jnp.sum(ls[jq, h, rows], axis=1, keepdims=True)).astype(jnp.bfloat16)
                for h in range(2)
            ]
            o_send[k, 0:S, r * D:(r + 1) * D] = jnp.where(flip, ends[1], ends[0])
            o_send[k, S:2 * S, r * D:(r + 1) * D] = jnp.where(flip, ends[0], ends[1])

    def finish_step(k, _):
        finish(k)
        o_copy(k).start()
        return 0

    lax.fori_loop(1, G, finish_step, 0)
    finish(0)
    mine = pltpu.make_async_copy(
        o_send.at[0], out_hbm.at[:, pl.ds(pl.multiple_of(ji * qw, qw), qw)], o_lsem
    )
    mine.start()

    for i, k in enumerate(order):
        part_copy(i).wait_send()
        if k:
            a2a_copy(i, k).wait_send()
            for h in range(2):
                q_copy(k, h).wait_send()
    for s in range(half_ring):
        for j in range(G):
            jj = (ji + j) % G
            ring_done((zi + B - s) % B, jj, s, 0)
            ring_done((zi + s) % B, jj, s, 1)
    for k in range(1, G):
        o_copy(k).wait_send()
        o_copy(k).wait_recv()
    mine.wait()


def body(hidden_states, queries, key_matrix, value_matrix, stretch_table):
    tokens, width = hidden_states.shape
    G = KEY_VALUE_HEADS // lax.axis_size("tp")
    ctx = lax.axis_size("ctx")
    B = ctx // G
    S = tokens // 2
    R = queries.shape[1] // (G * D)
    any_ = pl.BlockSpec(memory_space=pl.ANY)
    bf, f32 = jnp.bfloat16, jnp.float32
    dma = pltpu.SemaphoreType.DMA
    return pl.pallas_call(
        functools.partial(kernel, G, R, B, S),
        out_shape=jax.ShapeDtypeStruct(queries.shape, bf),
        in_specs=[pl.BlockSpec(memory_space=pltpu.SMEM)] + [any_] * 4,
        out_specs=any_,
        scratch_shapes=[
            pltpu.VMEM((tokens, width), bf),
            pltpu.VMEM((2 * G, width, 2 * D), bf),
            pltpu.VMEM((G, tokens, 2 * D), f32),
            pltpu.VMEM((G, tokens, 2 * D), f32),
            pltpu.VMEM((G, 2, 2, S, D), bf),
            pltpu.VMEM((B, G, 2, 2, S, D), bf),
            pltpu.VMEM((G, 2, S, R * D), bf),
            pltpu.VMEM((G, 2, R * S, D), bf),
            pltpu.VMEM((2, G * S, D), bf),
            pltpu.VMEM((2, G * S, D), bf),
            pltpu.VMEM((G, 2, R * S, D), f32),
            pltpu.VMEM((G, 2, R * S, D), f32),
            pltpu.VMEM((G, 2, R * S, D), f32),
            pltpu.VMEM((G, tokens, R * D), bf),
            dma,
            dma((2 * G, 2)),
            dma((G,)),
            dma((G,)),
            dma((G,)),
            dma((B, G)),
            dma((2, B // 2, G)),
            dma((G, 2)),
            dma((G, 2)),
            dma((2,)),
            dma((G,)),
            dma((G,)),
            dma,
        ],
        compiler_params=pltpu.CompilerParams(
            collective_id=0, has_side_effects=True, vmem_limit_bytes=60 * 1024 * 1024
        ),
        name="fused",
    )(stretch_table, hidden_states, queries, key_matrix, value_matrix)


def solution(mesh):
    in_specs = (P("ctx", "tp"), P("ctx", "tp"), P("tp", None), P("tp", None), P())
    out_specs = P("ctx", "tp")
    return jax.shard_map(body, mesh=mesh, in_specs=in_specs, out_specs=out_specs, check_vma=False)
```
